8 devices in a mesh: replica: 1 (over z), ep: 8 (over y, x, core).
Axes of the slice: x: 2, y: 2, z: 1, core: 2. Of those that a mesh axis runs over, the one named last changes fastest.
Arguments:
- tok_in: bfloat16 [4096, 2048], P(('replica', 'ep'))
- routes: int32 [2, 4096, 8], P(None, ('replica', 'ep'))
- gate_vals: float32 [2, 4096, 8], P(None, ('replica', 'ep'))
- w_gate: bfloat16 [2, 16, 2048, 1024], P(None, ('replica', 'ep'))
- w_up: bfloat16 [2, 16, 2048, 1024], P(None, ('replica', 'ep'))
- w_down: bfloat16 [2, 16, 1024, 2048], P(None, ('replica', 'ep'))
- sh_gate: bfloat16 [2, 2048, 1024], replicated
- sh_up: bfloat16 [2, 2048, 1024], replicated
- sh_down: bfloat16 [2, 1024, 2048], replicated
- old_map: int32 [2, 16], P(None, 'replica')
- move_slot: int32 [2, 2], P(None, 'replica')
- move_expert: int32 [2, 2], P(None, 'replica')
Outputs:
- output 1: bfloat16 [4096, 2048], P(('replica', 'ep'))
- output 2: bfloat16 [2, 16, 2048, 1024], P(None, ('replica', 'ep'))
- output 3: bfloat16 [2, 16, 2048, 1024], P(None, ('replica', 'ep'))
- output 4: bfloat16 [2, 16, 1024, 2048], P(None, ('replica', 'ep'))
All inputs are finite; a program needn't handle non-finite values.
Results may differ from the reference program's by a relative error of at most 0.0116165.
Values are sent between devices in bfloat16 or wider.
A program may use at most 1 GiB of HBM per device.

```python
import jax
import jax.numpy as jnp
from jax import lax

HIDDEN = 2048
EXPERT_FF = 1024
SHARED_FF = 1024
TOP_K = 8
GROUP_DEVS = 8
SLOTS_DEV = 2
TOKENS_DEV = 512
MOVE_COUNT = 2
EXPERTS = 12

SLOT_COUNT = GROUP_DEVS * SLOTS_DEV
TOKEN_COUNT = GROUP_DEVS * TOKENS_DEV
SCORE_RANGE = 2 ** 10
HOT_BONUS = 2 ** 9
COVER_BONUS = 2 ** 12


def draw_layout(rng_key):
    perm_key, extra_key, place_key = jax.random.split(rng_key, 3)
    expert_perm = jax.random.permutation(perm_key, EXPERTS).astype(jnp.int32)
    extra_slot = jax.random.randint(extra_key, (SLOT_COUNT - EXPERTS,), 0, EXPERTS, dtype=jnp.int32)
    canon_old = jnp.concatenate([expert_perm, extra_slot])
    cycled = jnp.concatenate([expert_perm[1:MOVE_COUNT], expert_perm[:1]])
    slot_perm = jax.random.permutation(place_key, SLOT_COUNT).astype(jnp.int32)
    old_map = canon_old[slot_perm]
    slot_of_canon = jnp.argsort(slot_perm).astype(jnp.int32)
    return old_map, slot_of_canon[:MOVE_COUNT], cycled, expert_perm[:MOVE_COUNT]


def draw_routes(rng_key, hot_ids):
    score_key, offset_key = jax.random.split(rng_key)
    score_int = jax.random.randint(score_key, (TOKEN_COUNT, EXPERTS), 0, SCORE_RANGE, dtype=jnp.int32)
    expert_ids = jnp.arange(EXPERTS, dtype=jnp.int32)
    is_hot = jnp.any(expert_ids[:, None] == hot_ids[None, :], axis=1).astype(jnp.int32)
    offset = jax.random.randint(offset_key, (), 0, EXPERTS, dtype=jnp.int32)
    token_ids = jnp.arange(TOKEN_COUNT, dtype=jnp.int32)
    cover_mask = ((token_ids[:, None] + offset) % EXPERTS == expert_ids[None, :]).astype(jnp.int32)
    total_score = score_int + HOT_BONUS * is_hot[None, :] + COVER_BONUS * cover_mask
    picked = lax.top_k(total_score * EXPERTS + expert_ids[None, :], TOP_K)[1]
    return picked.astype(jnp.int32)


def place_slots(expert_w, slot_map):
    return jnp.take(expert_w, slot_map, axis=0)


def setup_inputs(seed: int = 0, part: int = 0) -> dict:
    base_key = jax.random.key(seed)
    part_key = jax.random.fold_in(base_key, part)
    draw_keys = jax.random.split(part_key, 7)
    shared_keys = jax.random.split(jax.random.key(seed + 1), 3)
    old_map, move_slot, move_expert, hot_ids = jax.vmap(draw_layout)(jax.random.split(draw_keys[0], 2))
    routes = jax.vmap(draw_routes)(jax.random.split(draw_keys[1], 2), hot_ids)
    gate_vals = (0.5 + jax.random.uniform(draw_keys[2], (2, TOKEN_COUNT, TOP_K))) / TOP_K ** 0.5
    tok_in = jax.random.normal(draw_keys[3], (TOKEN_COUNT, HIDDEN)).astype(jnp.bfloat16)
    gate_e = (jax.random.normal(draw_keys[4], (2, EXPERTS, HIDDEN, EXPERT_FF)) * HIDDEN ** -0.5).astype(jnp.bfloat16)
    up_e = (jax.random.normal(draw_keys[5], (2, EXPERTS, HIDDEN, EXPERT_FF)) * HIDDEN ** -0.5).astype(jnp.bfloat16)
    down_e = (jax.random.normal(draw_keys[6], (2, EXPERTS, EXPERT_FF, HIDDEN)) * EXPERT_FF ** -0.5).astype(jnp.bfloat16)
    sh_gate = (jax.random.normal(shared_keys[0], (2, HIDDEN, SHARED_FF)) * HIDDEN ** -0.5).astype(jnp.bfloat16)
    sh_up = (jax.random.normal(shared_keys[1], (2, HIDDEN, SHARED_FF)) * HIDDEN ** -0.5).astype(jnp.bfloat16)
    sh_down = (jax.random.normal(shared_keys[2], (2, SHARED_FF, HIDDEN)) * SHARED_FF ** -0.5).astype(jnp.bfloat16)
    return {
        'tok_in': tok_in,
        'routes': routes,
        'gate_vals': gate_vals,
        'w_gate': jax.vmap(place_slots)(gate_e, old_map),
        'w_up': jax.vmap(place_slots)(up_e, old_map),
        'w_down': jax.vmap(place_slots)(down_e, old_map),
        'sh_gate': sh_gate,
        'sh_up': sh_up,
        'sh_down': sh_down,
        'old_map': old_map,
        'move_slot': move_slot,
        'move_expert': move_expert,
    }


def first_holder(slot_map, wanted):
    slot_ids = jnp.arange(SLOT_COUNT, dtype=jnp.int32)
    hit_mask = slot_map[None, :] == wanted[:, None]
    return jnp.min(jnp.where(hit_mask, slot_ids[None, :], SLOT_COUNT), axis=1)


def swiglu(hidden, w_gate, w_up, w_down):
    gate_proj = jnp.dot(hidden, w_gate, preferred_element_type=jnp.float32)
    up_proj = jnp.dot(hidden, w_up, preferred_element_type=jnp.float32)
    inner_act = (jax.nn.silu(gate_proj) * up_proj).astype(jnp.bfloat16)
    return jnp.dot(inner_act, w_down, preferred_element_type=jnp.float32)


def moe_layer(hidden, route_ids, gate_w, w_gate, w_up, w_down, sh_gate, sh_up, sh_down, slot_map):
    expert_ids = jnp.arange(EXPERTS, dtype=jnp.int32)
    holders = first_holder(slot_map, expert_ids)

    def add_expert(running, expert_idx):
        holder_slot = holders[expert_idx]
        expert_out = swiglu(hidden, w_gate[holder_slot], w_up[holder_slot], w_down[holder_slot])
        gate_col = jnp.sum(jnp.where(route_ids == expert_idx, gate_w, 0.0), axis=1)
        return running + gate_col[:, None] * expert_out, None

    start_acc = hidden.astype(jnp.float32) + swiglu(hidden, sh_gate, sh_up, sh_down)
    total_out = lax.scan(add_expert, start_acc, expert_ids)[0]
    return total_out.astype(jnp.bfloat16)


def reference(tok_in, routes, gate_vals, w_gate, w_up, w_down, sh_gate, sh_up, sh_down, old_map, move_slot, move_expert):
    hidden = tok_in
    new_sets = []
    for layer_idx in range(2):
        hidden = moe_layer(hidden, routes[layer_idx], gate_vals[layer_idx], w_gate[layer_idx], w_up[layer_idx], w_down[layer_idx], sh_gate[layer_idx], sh_up[layer_idx], sh_down[layer_idx], old_map[layer_idx])
        new_map = old_map[layer_idx].at[move_slot[layer_idx]].set(move_expert[layer_idx])
        source = first_holder(old_map[layer_idx], new_map)
        new_sets.append((jnp.take(w_gate[layer_idx], source, axis=0), jnp.take(w_up[layer_idx], source, axis=0), jnp.take(w_down[layer_idx], source, axis=0)))
    new_gate = jnp.stack([new_sets[0][0], new_sets[1][0]])
    new_up = jnp.stack([new_sets[0][1], new_sets[1][1]])
    new_down = jnp.stack([new_sets[0][2], new_sets[1][2]])
    return (hidden, new_gate, new_up, new_down)
```

```python
import functools

import jax
import jax.numpy as jnp
from jax import lax
from jax.experimental import pallas as pl
from jax.experimental.pallas import tpu as pltpu
from jax.sharding import PartitionSpec as P

TOKEN_AXES = ('replica', 'ep')
MESH = pl.DeviceIdType.MESH
F_TILE = 512
N_TILE = 1024


def first_holder(slot_map, wanted):
    slot_ids = jnp.arange(slot_map.shape[0], dtype=jnp.int32)
    hit_mask = slot_map[None, :] == wanted[:, None]
    return jnp.min(jnp.where(hit_mask, slot_ids[None, :], slot_map.shape[0]), axis=1)


def send_moved(weights, slot_map, move_expert, slots_dev, my_dev):
    source = first_holder(slot_map, move_expert)
    is_source = (source // slots_dev) == my_dev
    local_idx = source % slots_dev
    return tuple(jnp.where(is_source[:, None, None], jnp.take(weight_arr, local_idx, axis=0), jnp.zeros((), weight_arr.dtype)) for weight_arr in weights)


def place_moved(weights, arrived, move_slot, slots_dev, my_dev):
    local_ids = my_dev * slots_dev + jnp.arange(slots_dev, dtype=jnp.int32)
    match_mask = (move_slot[None, :] == local_ids[:, None]).astype(jnp.int32)
    is_target = jnp.max(match_mask, axis=1) > 0
    pick_idx = jnp.argmax(match_mask, axis=1)
    return tuple(jnp.where(is_target[:, None, None], jnp.take(arrived_arr, pick_idx, axis=0), weight_arr) for arrived_arr, weight_arr in zip(arrived, weights))


def slot_coefs(routes, gates, slot_map, slots_dev, my_dev):
    slot_ids = jnp.arange(slot_map.shape[0], dtype=jnp.int32)
    serve = (first_holder(slot_map, slot_map) == slot_ids).astype(jnp.float32)
    hit_mask = routes[:, :, None] == slot_map[None, None, :]
    coef = jnp.sum(jnp.where(hit_mask, gates[:, :, None], 0.0), axis=1) * serve[None, :]
    coef = coef.T.reshape(-1, 2, slots_dev, routes.shape[0])
    core = my_dev % 2
    coef = jnp.where(core == 0, coef, coef[:, ::-1])
    coef = coef.reshape(coef.shape[0], 2 * slots_dev, routes.shape[0])
    return jnp.pad(coef, ((0, 0), (0, 8 - 2 * slots_dev), (0, 0)))


def layer_kernel(layer, h_ref, ct_ref, wg_ref, wu_ref, wd_ref, sg_ref, su_ref, sd_ref,
                 out_ref, xg_ref, pout_ref, hs_ref, rcv_ref,
                 wg_v, wu_v, wd_v, xbuf, pbuf, ab, obuf, cbuf, ccol, send_sem, recv_sem, loc_sem):
    me = lax.axis_index('ep')
    core = me % 2
    x = (me // 2) % 2
    y = me // 4
    chip = me // 2
    to_core = me + 1 - 2 * core
    to_x = me + 2 - 4 * x
    to_y = me + 4 - 8 * y
    to_d = me + 6 - 4 * x - 8 * y
    rows = xbuf.shape[0]
    half = rows // 2

    def remote(i, src, dst, dev):
        return pltpu.make_async_remote_copy(src_ref=src, dst_ref=dst, send_sem=send_sem.at[i], recv_sem=recv_sem.at[i], device_id={'ep': dev}, device_id_type=MESH)

    def local(i, src, dst):
        return pltpu.make_async_copy(src, dst, loc_sem.at[i])

    own_a, own_b = h_ref.at[pl.ds(0, rows)], h_ref.at[pl.ds(rows, rows)]
    lo, hi = pl.ds(0, half), pl.ds(half, half)
    ag = [
        remote(0, own_a, xg_ref.at[0], to_x),
        remote(1, own_b, xg_ref.at[1], to_y),
        remote(2, xg_ref.at[0], xg_ref.at[2], to_y),
        remote(3, xg_ref.at[1], xg_ref.at[3], to_x),
        remote(4, own_b, xg_ref.at[4], to_x),
        remote(5, own_a, xg_ref.at[5], to_y),
    ]
    cs = [
        remote(6, ct_ref.at[(chip + 1 - 2 * x)], cbuf.at[1], to_x),
        remote(7, ct_ref.at[(chip + 2 - 4 * y)], cbuf.at[2], to_y),
        remote(8, ct_ref.at[(chip + 3 - 2 * x - 4 * y)], cbuf.at[3], to_d),
    ]
    ws = [
        remote(9, wg_ref.at[layer], wg_v.at[pl.ds(2, 2)], to_core),
        remote(10, wu_ref.at[layer], wu_v.at[pl.ds(2, 2)], to_core),
        remote(11, wd_ref.at[layer], wd_v.at[pl.ds(2, 2)], to_core),
    ]
    s_xa = remote(12, pout_ref.at[0], rcv_ref.at[0], to_x)
    s_da = [remote(13, pout_ref.at[2, lo], rcv_ref.at[1, lo], to_x), remote(14, pout_ref.at[2, hi], rcv_ref.at[1, hi], to_x)]
    s_yb = remote(15, pout_ref.at[1], rcv_ref.at[2], to_y)
    s_db = [remote(16, pout_ref.at[3, lo], rcv_ref.at[3, lo], to_y), remote(17, pout_ref.at[3, hi], rcv_ref.at[3, hi], to_y)]
    s_xb = [remote(18, pout_ref.at[4, lo], rcv_ref.at[4, lo], to_x), remote(19, pout_ref.at[4, hi], rcv_ref.at[4, hi], to_x)]
    s_ya = [remote(20, pout_ref.at[5, lo], rcv_ref.at[5, lo], to_y), remote(21, pout_ref.at[5, hi], rcv_ref.at[5, hi], to_y)]

    barrier = pltpu.get_barrier_semaphore()
    for dev in (to_core, to_x, to_y, to_d):
        pl.semaphore_signal(barrier, inc=1, device_id={'ep': dev}, device_id_type=MESH)
    pl.semaphore_wait(barrier, 4)

    for c in cs:
        c.start()
    for i in (0, 1, 4, 5):
        ag[i].start()
    for c in ws:
        c.start()

    shared_in = [local(0, sg_ref.at[layer], wg_v.at[1]), local(1, su_ref.at[layer], wu_v.at[1]), local(2, sd_ref.at[layer], wd_v.at[1])]
    first_in = [local(3, wg_ref.at[layer, 0], wg_v.at[0]), local(4, wu_ref.at[layer, 0], wu_v.at[0]), local(5, wd_ref.at[layer, 0], wd_v.at[0])]
    second_in = [local(0, wg_ref.at[layer, 1], wg_v.at[1]), local(1, wu_ref.at[layer, 1], wu_v.at[1]), local(2, wd_ref.at[layer, 1], wd_v.at[1])]
    coef_in = local(6, ct_ref.at[chip], cbuf.at[0])
    for c in shared_in:
        c.start()
    for c in first_in:
        c.start()
    coef_in.start()

    def expert(slot, acc, coef):
        def f_step(ft, carry):
            cols = pl.ds(pl.multiple_of(ft * F_TILE, F_TILE), F_TILE)
            tok = xbuf[...]
            gate_proj = jnp.dot(tok, wg_v[slot, :, cols], preferred_element_type=jnp.float32)
            up_proj = jnp.dot(tok, wu_v[slot, :, cols], preferred_element_type=jnp.float32)
            inner = (jax.nn.silu(gate_proj) * up_proj).astype(jnp.bfloat16)
            for n in range(acc.shape[1] // N_TILE):
                ns = pl.ds(n * N_TILE, N_TILE)
                part = jnp.dot(inner, wd_v[slot, cols, ns], preferred_element_type=jnp.float32)
                acc[:, ns] += part if coef is None else coef * part
            return carry
        lax.fori_loop(0, wg_v.shape[2] // F_TILE, f_step, 0)

    for c in shared_in:
        c.wait()

    def shared_step(p, carry):
        src = h_ref.at[pl.ds(pl.multiple_of(p * rows, rows), rows)]
        load = local(7, src, xbuf)
        load.start()
        load.wait()
        acc = pbuf.at[0]
        acc[...] = xbuf[...].astype(jnp.float32)
        expert(1, acc, None)
        store = local(7, acc, hs_ref.at[p])
        store.start()
        store.wait()
        return carry
    lax.fori_loop(0, 2, shared_step, 0)
    for c in second_in:
        c.start()

    ag[0].wait_recv()
    ag[2].start()
    ag[1].wait_recv()
    ag[3].start()

    for c in cs:
        c.wait_recv()
    coef_in.wait()
    for k, (rel, part) in enumerate([(1, 0), (2, 1), (3, 0), (3, 1), (1, 1), (2, 0), (0, 0), (0, 1)]):
        ccol[k, :, pl.ds(0, 8)] = jnp.transpose(cbuf[rel, :, pl.ds(part * rows, rows)])
    for c in second_in + first_in:
        c.wait()
    for c in ws:
        c.wait_recv()

    def add_half(h):
        part = lo if h == 0 else hi
        for mine, theirs, arrived, out in ((4, 3, s_db[h], s_xb[h]), (5, 1, s_da[h], s_ya[h])):
            load_a = local(0, pout_ref.at[mine, part], ab.at[0])
            load_a.start()
            arrived.wait_recv()
            load_b = local(1, rcv_ref.at[theirs, part], ab.at[1])
            load_b.start()
            load_a.wait()
            load_b.wait()
            ab[0] = ab[0] + ab[1]
            store = local(0, ab.at[0], pout_ref.at[mine, part])
            store.start()
            store.wait()
            out.start()

    def step(k, carry):
        for j in range(2, 6):
            @pl.when(k == j)
            def _():
                ag[j].wait_recv()
        acc = pbuf.at[k % 2]

        @pl.when(k < 6)
        def _():
            load = local(7, xg_ref.at[lax.rem(k, 6)], xbuf)
            load.start()
            acc[...] = jnp.zeros_like(acc)
            load.wait()

        @pl.when(k >= 6)
        def _():
            p = k % 2
            load = local(7, h_ref.at[pl.ds(pl.multiple_of(p * rows, rows), rows)], xbuf)
            load_s = local(6, hs_ref.at[p], acc)
            load.start()
            load_s.start()
            load.wait()
            load_s.wait()

        def slot_step(slot, c):
            coefs = ccol[k, :, pl.ds(0, 8)]
            lane = lax.broadcasted_iota(jnp.int32, coefs.shape, 1)
            col = jnp.sum(jnp.where(lane == slot, coefs, 0.0), axis=1, keepdims=True)
            expert(slot, acc, col)
            return c
        lax.fori_loop(0, wg_v.shape[0], slot_step, 0)

        @pl.when(k < 6)
        def _():
            store = local(7, acc, pout_ref.at[lax.rem(k, 6)])
            store.start()
            store.wait()
        for j, outs in ((0, [s_xa]), (1, [s_yb]), (2, s_da), (3, s_db)):
            @pl.when(k == j)
            def _():
                for c in outs:
                    c.start()
        for j, h in ((5, 0), (6, 1)):
            @pl.when(k == j)
            def _():
                add_half(h)
        return carry
    lax.fori_loop(0, 8, step, 0)

    s_xa.wait_recv()
    s_yb.wait_recv()
    for h, part in enumerate((lo, hi)):
        loads = [local(0, rcv_ref.at[0, part], ab.at[0]), local(1, rcv_ref.at[2, part], ab.at[1])]
        for c in loads:
            c.start()
        for i, c in enumerate(loads):
            c.wait()
            pbuf[i, part] = pbuf[i, part] + ab[i]
    stores = []
    for h, part in enumerate((lo, hi)):
        loads = []
        for i, (arrived, src) in enumerate(((s_ya[h], 5), (s_xb[h], 4))):
            arrived.wait_recv()
            load = local(i, rcv_ref.at[src, part], ab.at[i])
            load.start()
            loads.append(load)
        for i, c in enumerate(loads):
            c.wait()
            obuf[2 * h + i] = (pbuf[i, part] + ab[i]).astype(jnp.bfloat16)
            store = local(2 + 2 * h + i, obuf.at[2 * h + i], out_ref.at[pl.ds(i * rows + h * half, half)])
            store.start()
            stores.append(store)
    for c in stores:
        c.wait()
    for c in ag + cs + ws + [s_xa, s_yb] + s_da + s_db + s_xb + s_ya:
        c.wait_send()


def moe_layer(layer, hidden, coefs, weights, shared):
    tokens, width = hidden.shape
    inner = weights[0].shape[3]
    rows = tokens // 2
    f32, bf16 = jnp.float32, jnp.bfloat16
    any_spec = pl.BlockSpec(memory_space=pl.ANY)
    flops = 2 * 3 * width * inner * (4 * 4 * tokens + tokens)
    outs = pl.pallas_call(
        functools.partial(layer_kernel, layer),
        out_shape=(
            jax.ShapeDtypeStruct((tokens, width), bf16),
            jax.ShapeDtypeStruct((6, rows, width), bf16),
            jax.ShapeDtypeStruct((6, rows, width), f32),
            jax.ShapeDtypeStruct((2, rows, width), f32),
            jax.ShapeDtypeStruct((6, rows, width), f32),
        ),
        in_specs=[any_spec] * 8,
        out_specs=[any_spec] * 5,
        scratch_shapes=[
            pltpu.VMEM((4, width, inner), bf16),
            pltpu.VMEM((4, width, inner), bf16),
            pltpu.VMEM((4, inner, width), bf16),
            pltpu.VMEM((rows, width), bf16),
            pltpu.VMEM((2, rows, width), f32),
            pltpu.VMEM((2, rows // 2, width), f32),
            pltpu.VMEM((4, rows // 2, width), bf16),
            pltpu.VMEM((4, 8, tokens), f32),
            pltpu.VMEM((8, rows, 128), f32),
            pltpu.SemaphoreType.DMA((22,)),
            pltpu.SemaphoreType.DMA((22,)),
            pltpu.SemaphoreType.DMA((8,)),
        ],
        compiler_params=pltpu.CompilerParams(collective_id=layer, has_side_effects=True, vmem_limit_bytes=67043328),
        cost_estimate=pl.CostEstimate(flops=flops, bytes_accessed=200 * 2 ** 20, transcendentals=0),
        name=f'moe_layer_{layer}',
    )(hidden, coefs, *weights, *shared)
    return outs[0]


def solution(mesh):
    def body(tok_in, routes, gate_vals, w_gate, w_up, w_down, sh_gate, sh_up, sh_down, old_map, move_slot, move_expert):
        my_dev = lax.axis_index('ep')
        slots_dev = w_gate.shape[1]
        hidden = tok_in
        placed = []
        for layer_idx in range(2):
            layer_w = (w_gate[layer_idx], w_up[layer_idx], w_down[layer_idx])
            outgoing = send_moved(layer_w, old_map[layer_idx], move_expert[layer_idx], slots_dev, my_dev)
            arrived = lax.psum(outgoing, 'ep')
            placed.append(place_moved(layer_w, arrived, move_slot[layer_idx], slots_dev, my_dev))
        for layer_idx in range(2):
            coefs = slot_coefs(routes[layer_idx], gate_vals[layer_idx], old_map[layer_idx], slots_dev, my_dev)
            hidden = moe_layer(layer_idx, hidden, coefs, (w_gate, w_up, w_down), (sh_gate, sh_up, sh_down))
        new_gate = jnp.stack([placed[0][0], placed[1][0]])
        new_up = jnp.stack([placed[0][1], placed[1][1]])
        new_down = jnp.stack([placed[0][2], placed[1][2]])
        return (hidden, new_gate, new_up, new_down)

    weight_spec = P(None, TOKEN_AXES, None, None)
    route_spec = P(None, TOKEN_AXES, None)
    map_spec = P(None, 'replica')
    shared_spec = P(None, None, None)
    tok_spec = P(TOKEN_AXES, None)
    return jax.shard_map(body, mesh=mesh, in_specs=(tok_spec, route_spec, route_spec, weight_spec, weight_spec, weight_spec, shared_spec, shared_spec, shared_spec, map_spec, map_spec, map_spec), out_specs=(tok_spec, weight_spec, weight_spec, weight_spec), check_vma=False)
```

```python
import functools

import jax
import jax.numpy as jnp
from jax import lax
from jax.experimental import pallas as pl
from jax.experimental.pallas import tpu as pltpu
from jax.sharding import PartitionSpec as P

TOKEN_AXES = ('replica', 'ep')
MESH = pl.DeviceIdType.MESH
F_TILE = 512
N_TILE = 1024


def first_holder(slot_map, wanted):
    slot_ids = jnp.arange(slot_map.shape[0], dtype=jnp.int32)
    hit_mask = slot_map[None, :] == wanted[:, None]
    return jnp.min(jnp.where(hit_mask, slot_ids[None, :], slot_map.shape[0]), axis=1)


def send_moved(weights, slot_map, move_expert, slots_dev, my_dev):
    source = first_holder(slot_map, move_expert)
    is_source = (source // slots_dev) == my_dev
    local_idx = source % slots_dev
    return tuple(jnp.where(is_source[:, None, None], jnp.take(weight_arr, local_idx, axis=0), jnp.zeros((), weight_arr.dtype)) for weight_arr in weights)


def place_moved(weights, arrived, move_slot, slots_dev, my_dev):
    local_ids = my_dev * slots_dev + jnp.arange(slots_dev, dtype=jnp.int32)
    match_mask = (move_slot[None, :] == local_ids[:, None]).astype(jnp.int32)
    is_target = jnp.max(match_mask, axis=1) > 0
    pick_idx = jnp.argmax(match_mask, axis=1)
    return tuple(jnp.where(is_target[:, None, None], jnp.take(arrived_arr, pick_idx, axis=0), weight_arr) for arrived_arr, weight_arr in zip(arrived, weights))


def slot_coefs(routes, gates, slot_map, slots_dev, my_dev):
    slot_ids = jnp.arange(slot_map.shape[0], dtype=jnp.int32)
    serve = (first_holder(slot_map, slot_map) == slot_ids).astype(jnp.float32)
    hit_mask = routes[:, :, None] == slot_map[None, None, :]
    coef = jnp.sum(jnp.where(hit_mask, gates[:, :, None], 0.0), axis=1) * serve[None, :]
    coef = coef.T.reshape(-1, 2, slots_dev, routes.shape[0])
    core = my_dev % 2
    coef = jnp.where(core == 0, coef, coef[:, ::-1])
    coef = coef.reshape(coef.shape[0], 2 * slots_dev, routes.shape[0])
    return jnp.pad(coef, ((0, 0), (0, 8 - 2 * slots_dev), (0, 0)))


def layer_kernel(layer, h_ref, ct_ref, wg_ref, wu_ref, wd_ref, sg_ref, su_ref, sd_ref,
                 out_ref, xg_ref, pout_ref, hs_ref, rcv_ref,
                 wg_v, wu_v, wd_v, xbuf, pbuf, ab, obuf, cbuf, ccol, send_sem, recv_sem, loc_sem):
    me = lax.axis_index('ep')
    core = me % 2
    x = (me // 2) % 2
    y = me // 4
    chip = me // 2
    to_core = me + 1 - 2 * core
    to_x = me + 2 - 4 * x
    to_y = me + 4 - 8 * y
    to_d = me + 6 - 4 * x - 8 * y
    rows = xbuf.shape[0]
    half = rows // 2

    def remote(i, src, dst, dev):
        return pltpu.make_async_remote_copy(src_ref=src, dst_ref=dst, send_sem=send_sem.at[i], recv_sem=recv_sem.at[i], device_id={'ep': dev}, device_id_type=MESH)

    def local(i, src, dst):
        return pltpu.make_async_copy(src, dst, loc_sem.at[i])

    own_a, own_b = h_ref.at[pl.ds(0, rows)], h_ref.at[pl.ds(rows, rows)]
    lo, hi = pl.ds(0, half), pl.ds(half, half)
    ag = [
        remote(0, own_a, xg_ref.at[0], to_x),
        remote(1, own_b, xg_ref.at[1], to_y),
        remote(2, xg_ref.at[0], xg_ref.at[2], to_y),
        remote(3, xg_ref.at[1], xg_ref.at[3], to_x),
        remote(4, own_b, xg_ref.at[4], to_x),
        remote(5, own_a, xg_ref.at[5], to_y),
    ]
    cs = [
        remote(6, ct_ref.at[(chip + 1 - 2 * x)], cbuf.at[1], to_x),
        remote(7, ct_ref.at[(chip + 2 - 4 * y)], cbuf.at[2], to_y),
        remote(8, ct_ref.at[(chip + 3 - 2 * x - 4 * y)], cbuf.at[3], to_d),
    ]
    ws = [
        remote(9, wg_ref.at[layer], wg_v.at[pl.ds(2, 2)], to_core),
        remote(10, wu_ref.at[layer], wu_v.at[pl.ds(2, 2)], to_core),
        remote(11, wd_ref.at[layer], wd_v.at[pl.ds(2, 2)], to_core),
    ]
    s_xa = remote(12, pout_ref.at[0], rcv_ref.at[0], to_x)
    s_da = [remote(13, pout_ref.at[2, lo], rcv_ref.at[1, lo], to_x), remote(14, pout_ref.at[2, hi], rcv_ref.at[1, hi], to_x)]
    s_yb = remote(15, pout_ref.at[1], rcv_ref.at[2], to_y)
    s_db = [remote(16, pout_ref.at[3, lo], rcv_ref.at[3, lo], to_y), remote(17, pout_ref.at[3, hi], rcv_ref.at[3, hi], to_y)]
    s_xb = [remote(18, pout_ref.at[4, lo], rcv_ref.at[4, lo], to_x), remote(19, pout_ref.at[4, hi], rcv_ref.at[4, hi], to_x)]
    s_ya = [remote(20, pout_ref.at[5, lo], rcv_ref.at[5, lo], to_y), remote(21, pout_ref.at[5, hi], rcv_ref.at[5, hi], to_y)]

    barrier = pltpu.get_barrier_semaphore()
    for dev in (to_core, to_x, to_y, to_d):
        pl.semaphore_signal(barrier, inc=1, device_id={'ep': dev}, device_id_type=MESH)
    pl.semaphore_wait(barrier, 4)

    for c in cs:
        c.start()
    for i in (0, 1, 4, 5):
        ag[i].start()
    for c in ws:
        c.start()

    shared_in = [local(0, sg_ref.at[layer], wg_v.at[1]), local(1, su_ref.at[layer], wu_v.at[1]), local(2, sd_ref.at[layer], wd_v.at[1])]
    first_in = [local(3, wg_ref.at[layer, 0], wg_v.at[0]), local(4, wu_ref.at[layer, 0], wu_v.at[0]), local(5, wd_ref.at[layer, 0], wd_v.at[0])]
    second_in = [local(0, wg_ref.at[layer, 1], wg_v.at[1]), local(1, wu_ref.at[layer, 1], wu_v.at[1]), local(2, wd_ref.at[layer, 1], wd_v.at[1])]
    coef_in = local(6, ct_ref.at[chip], cbuf.at[0])
    for c in shared_in:
        c.start()
    for c in first_in:
        c.start()
    coef_in.start()

    def expert(slot, acc, coef):
        def f_step(ft, carry):
            cols = pl.ds(pl.multiple_of(ft * F_TILE, F_TILE), F_TILE)
            tok = xbuf[...]
            gate_proj = jnp.dot(tok, wg_v[slot, :, cols], preferred_element_type=jnp.float32)
            up_proj = jnp.dot(tok, wu_v[slot, :, cols], preferred_element_type=jnp.float32)
            inner = (jax.nn.silu(gate_proj) * up_proj).astype(jnp.bfloat16)
            for n in range(acc.shape[1] // N_TILE):
                ns = pl.ds(n * N_TILE, N_TILE)
                part = jnp.dot(inner, wd_v[slot, cols, ns], preferred_element_type=jnp.float32)
                acc[:, ns] += part if coef is None else coef * part
            return carry
        lax.fori_loop(0, wg_v.shape[2] // F_TILE, f_step, 0)

    for c in shared_in:
        c.wait()

    def shared_step(p, carry):
        src = h_ref.at[pl.ds(pl.multiple_of(p * rows, rows), rows)]
        load = local(7, src, xbuf)
        load.start()
        load.wait()
        acc = pbuf.at[0]
        acc[...] = xbuf[...].astype(jnp.float32)
        expert(1, acc, None)
        store = local(7, acc, hs_ref.at[p])
        store.start()
        store.wait()
        return carry
    lax.fori_loop(0, 2, shared_step, 0)
    for c in second_in:
        c.start()

    ag[0].wait_recv()
    ag[2].start()
    ag[1].wait_recv()
    ag[3].start()

    for c in cs:
        c.wait_recv()
    coef_in.wait()
    for k, (rel, part) in enumerate([(1, 0), (2, 1), (3, 0), (3, 1), (1, 1), (2, 0), (0, 0), (0, 1)]):
        ccol[k, :, pl.ds(0, 8)] = jnp.transpose(cbuf[rel, :, pl.ds(part * rows, rows)])
    for c in second_in + first_in:
        c.wait()
    for c in ws:
        c.wait_recv()

    def add_half(h):
        part = lo if h == 0 else hi
        for mine, theirs, arrived, out in ((4, 3, s_db[h], s_xb[h]), (5, 1, s_da[h], s_ya[h])):
            load_a = local(0, pout_ref.at[mine, part], ab.at[0])
            load_a.start()
            arrived.wait_recv()
            load_b = local(1, rcv_ref.at[theirs, part], ab.at[1])
            load_b.start()
            load_a.wait()
            load_b.wait()
            ab[0] = ab[0] + ab[1]
            store = local(0, ab.at[0], pout_ref.at[mine, part])
            store.start()
            store.wait()
            out.start()

    def step(k, carry):
        for j in range(2, 6):
            @pl.when(k == j)
            def _():
                ag[j].wait_recv()
        acc = pbuf.at[k % 2]

        @pl.when(k < 6)
        def _():
            load = local(7, xg_ref.at[lax.rem(k, 6)], xbuf)
            load.start()
            acc[...] = jnp.zeros_like(acc)
            load.wait()

        @pl.when(k >= 6)
        def _():
            p = k % 2
            load = local(7, h_ref.at[pl.ds(pl.multiple_of(p * rows, rows), rows)], xbuf)
            load_s = local(6, hs_ref.at[p], acc)
            load.start()
            load_s.start()
            load.wait()
            load_s.wait()

        def slot_step(slot, c):
            coefs = ccol[k, :, pl.ds(0, 8)]
            lane = lax.broadcasted_iota(jnp.int32, coefs.shape, 1)
            col = jnp.sum(jnp.where(lane == slot, coefs, 0.0), axis=1, keepdims=True)
            expert(slot, acc, col)
            return c
        lax.fori_loop(0, wg_v.shape[0], slot_step, 0)

        @pl.when(k < 6)
        def _():
            store = local(7, acc, pout_ref.at[lax.rem(k, 6)])
            store.start()
            store.wait()
        for j, outs in ((0, [s_xa]), (1, [s_yb]), (2, s_da), (3, s_db)):
            @pl.when(k == j)
            def _():
                for c in outs:
                    c.start()
        for j, h in ((5, 0), (6, 1)):
            @pl.when(k == j)
            def _():
                add_half(h)
        return carry
    lax.fori_loop(0, 8, step, 0)

    s_xa.wait_recv()
    s_yb.wait_recv()
    for h, part in enumerate((lo, hi)):
        loads = [local(0, rcv_ref.at[0, part], ab.at[0]), local(1, rcv_ref.at[2, part], ab.at[1])]
        for c in loads:
            c.start()
        for i, c in enumerate(loads):
            c.wait()
            pbuf[i, part] = pbuf[i, part] + ab[i]
    stores = []
    for h, part in enumerate((lo, hi)):
        loads = []
        for i, (arrived, src) in enumerate(((s_ya[h], 5), (s_xb[h], 4))):
            arrived.wait_recv()
            load = local(i, rcv_ref.at[src, part], ab.at[i])
            load.start()
            loads.append(load)
        for i, c in enumerate(loads):
            c.wait()
            obuf[2 * h + i] = (pbuf[i, part] + ab[i]).astype(jnp.bfloat16)
            store = local(2 + 2 * h + i, obuf.at[2 * h + i], out_ref.at[pl.ds(i * rows + h * half, half)])
            store.start()
            stores.append(store)
    for c in stores:
        c.wait()
    for c in ag + cs + ws + [s_xa, s_yb] + s_da + s_db + s_xb + s_ya:
        c.wait_send()


def moe_layer(layer, hidden, coefs, weights, shared):
    tokens, width = hidden.shape
    inner = weights[0].shape[3]
    rows = tokens // 2
    f32, bf16 = jnp.float32, jnp.bfloat16
    any_spec = pl.BlockSpec(memory_space=pl.ANY)
    flops = 2 * 3 * width * inner * (4 * 4 * tokens + tokens)
    outs = pl.pallas_call(
        functools.partial(layer_kernel, layer),
        out_shape=(
            jax.ShapeDtypeStruct((tokens, width), bf16),
            jax.ShapeDtypeStruct((6, rows, width), bf16),
            jax.ShapeDtypeStruct((6, rows, width), f32),
            jax.ShapeDtypeStruct((2, rows, width), f32),
            jax.ShapeDtypeStruct((6, rows, width), f32),
        ),
        in_specs=[any_spec] * 8,
        out_specs=[any_spec] * 5,
        scratch_shapes=[
            pltpu.VMEM((4, width, inner), bf16),
            pltpu.VMEM((4, width, inner), bf16),
            pltpu.VMEM((4, inner, width), bf16),
            pltpu.VMEM((rows, width), bf16),
            pltpu.VMEM((2, rows, width), f32),
            pltpu.VMEM((2, rows // 2, width), f32),
            pltpu.VMEM((4, rows // 2, width), bf16),
            pltpu.VMEM((4, 8, tokens), f32),
            pltpu.VMEM((8, rows, 128), f32),
            pltpu.SemaphoreType.DMA((22,)),
            pltpu.SemaphoreType.DMA((22,)),
            pltpu.SemaphoreType.DMA((8,)),
        ],
        compiler_params=pltpu.CompilerParams(collective_id=layer, has_side_effects=True, vmem_limit_bytes=67043328),
        cost_estimate=pl.CostEstimate(flops=flops, bytes_accessed=200 * 2 ** 20, transcendentals=0),
        name=f'moe_layer_{layer}',
    )(hidden, coefs, *weights, *shared)
    return outs[0]


def move_plan(old_map, move_slot, move_expert, slots_dev, group, my_dev):
    layers = old_map.shape[0]
    devs = jnp.arange(group, dtype=jnp.int32)
    held = old_map.reshape(layers, group, slots_dev)
    dst = move_slot // slots_dev
    holds = jnp.any(held[:, None] == move_expert[:, :, None, None], axis=3)
    is_dst = devs[None, None, :] == dst[:, :, None]
    far = ~jnp.any(holds & is_dst, axis=2)
    diff = devs[None, None, :] ^ dst[:, :, None]
    hops = (diff & 1) + 4 * ((diff // 2) & 1) + 4 * (diff // 4)
    near = jnp.min(jnp.where(holds, hops, 64) * group + devs, axis=2) % group
    both = far[:, 0] & far[:, 1]
    swap_ok = jnp.all(jnp.any(holds & is_dst[:, ::-1], axis=2), axis=1)
    src = jnp.where(both[:, None], dst[:, ::-1], near)
    one = jnp.where(far[:, 0], 0, 1)
    pick = lambda a: jnp.where(one == 0, a[:, 0], a[:, 1])
    first, second = pick(src), pick(dst)
    low, high = jnp.minimum(first, second), jnp.maximum(first, second)
    pair = low * (2 * group - 1 - low) // 2 + high - low
    pair = jnp.where(far[:, 0] | far[:, 1], pair, 0)
    mine = jnp.sum(jnp.where((devs == my_dev)[None, :, None], held, 0), axis=1)
    sends = far & (src == my_dev)
    at_one = mine[:, None, 0] != move_expert
    sel = jnp.max((sends & at_one).astype(jnp.int32), axis=1)
    slots = my_dev * slots_dev + jnp.arange(slots_dev, dtype=jnp.int32)
    code = jnp.where(far, 2, 1)[:, :, None] * (move_slot[:, :, None] == slots[None, None, :]).astype(jnp.int32)
    return jnp.all(swap_ok | ~both), pair, sel, jnp.max(code, axis=1)


def device_paths(a, b):
    at = lambda y, x, c: (y * 2 + x) * 2 + c
    (ya, xa, ca), (yb, xb, cb) = [(d // 4, (d // 2) % 2, d % 2) for d in (a, b)]
    if (ya, xa) == (yb, xb):
        return [[a, b], [a, b]]
    if ya == yb:
        return [[a, b], [a, at(1 - ya, xa, ca), at(1 - yb, xb, cb), b]]
    if xa == xb:
        return [[a, b], [a, at(ya, 1 - xa, ca), at(yb, 1 - xb, cb), b]]
    return [[a, at(ya, xb, ca), b], [a, at(yb, xa, ca), b]]


def swap_kernel(layer, a, b, sel_ref, wg_ref, wu_ref, wd_ref, ag_ref, au_ref, ad_ref, pg_ref, pu_ref, pd_ref,
                relay_gu, relay_d, stage_gu, stage_d, send_sem, recv_sem, loc_sem):
    me = lax.axis_index('ep')
    paths = device_paths(a, b)
    weights, pays, arrs = (wg_ref, wu_ref, wd_ref), (pg_ref, pu_ref, pd_ref), (ag_ref, au_ref, ad_ref)
    per = 4

    def rows_of(n, route, i):
        size = arrs[n].shape[0] // (2 * per)
        start = route * (arrs[n].shape[0] // 2) + i * size
        return pl.ds(start if isinstance(start, int) else pl.multiple_of(start, size), size)

    def relay(n, way, i):
        return relay_d.at[way, i] if n == 2 else relay_gu.at[way, n * per + i]

    def hop(route, way, n, i, src, last, dev):
        dst = arrs[n].at[rows_of(n, route, i)] if last else relay(n, way, i)
        q = n * per + i
        return pltpu.make_async_remote_copy(src_ref=src, dst_ref=dst, send_sem=send_sem.at[route, way, q], recv_sem=recv_sem.at[route, way, q], device_id={'ep': dev}, device_id_type=MESH)

    @pl.when((me == a) | (me == b))
    def _():
        way = (me - a) // (b - a)

        def out(route, n, i):
            path = paths[route]
            dev = path[1] + way * (path[-2] - path[1])
            return hop(route, way, n, i, pays[n].at[rows_of(n, route, i)], len(path) == 2, dev)

        for n in range(3):
            stage = stage_d if n == 2 else stage_gu

            def send(i, carry):
                loads = [pltpu.make_async_copy(weights[n].at[layer, s, rows_of(n, route, i)], stage.at[route, s], loc_sem.at[2 * route + s]) for route in range(2) for s in range(2)]
                for c in loads:
                    c.start()
                for c in loads:
                    c.wait()
                stores = []
                for route in range(2):
                    stage[route, 0] = jnp.where(sel_ref[0] == 0, stage[route, 0], stage[route, 1])
                    store = pltpu.make_async_copy(stage.at[route, 0], pays[n].at[rows_of(n, route, i)], loc_sem.at[route])
                    store.start()
                    stores.append(store)
                for route in range(2):
                    stores[route].wait()
                    out(route, n, i).start()
                return carry
            lax.fori_loop(0, per, send, 0)
        for n in range(3):
            def finish(i, carry):
                for route in range(2):
                    hop(route, 1 - way, n, i, pays[n].at[rows_of(n, route, i)], True, me).wait_recv()
                    out(route, n, i).wait_send()
                return carry
            lax.fori_loop(0, per, finish, 0)

    for route, path in enumerate(paths):
        for h in range(1, len(path) - 1):
            @pl.when(me == path[h])
            def _():
                late = len(path) - 1 - 2 * h
                lags = (max(0, -late), max(0, late))
                sent = []
                for t in range(3 * per + max(lags)):
                    for way in range(2):
                        q = t - lags[way]
                        if 0 <= q < 3 * per:
                            n, i = q // per, q % per
                            nxt = path[h + 1] if way == 0 else path[h - 1]
                            fwd = hop(route, way, n, i, relay(n, way, i), nxt in (a, b), nxt)
                            hop(route, way, n, i, relay(n, way, i), False, nxt).wait_recv()
                            fwd.start()
                            sent.append(fwd)
                for c in sent:
                    c.wait_send()


def swap_call(layer, pair, sel, weights):
    rows_g, cols_g = weights[0].shape[2:]
    rows_d, cols_d = weights[2].shape[2:]
    dt = weights[0].dtype
    any_spec = pl.BlockSpec(memory_space=pl.ANY)
    arrays = tuple(jax.ShapeDtypeStruct(w.shape[2:], dt) for w in weights)
    if pair is None:
        return pl.pallas_call(lambda s, *refs: None, out_shape=arrays, in_specs=[pl.BlockSpec(memory_space=pltpu.SMEM)], out_specs=[any_spec] * 3, name='no_swap')(sel)
    return pl.pallas_call(
        functools.partial(swap_kernel, layer, *pair),
        out_shape=arrays + arrays,
        in_specs=[pl.BlockSpec(memory_space=pltpu.SMEM)] + [any_spec] * 3,
        out_specs=[any_spec] * 6,
        scratch_shapes=[
            pltpu.VMEM((2, 8, rows_g // 8, cols_g), dt),
            pltpu.VMEM((2, 4, rows_d // 8, cols_d), dt),
            pltpu.VMEM((2, 2, rows_g // 8, cols_g), dt),
            pltpu.VMEM((2, 2, rows_d // 8, cols_d), dt),
            pltpu.SemaphoreType.DMA((2, 2, 12)),
            pltpu.SemaphoreType.DMA((2, 2, 12)),
            pltpu.SemaphoreType.DMA((4,)),
        ],
        compiler_params=pltpu.CompilerParams(has_side_effects=True),
        name=f'swap_{layer}_{pair[0]}_{pair[1]}',
    )(sel, *weights)[:3]


def place_kernel(code_ref, *refs):
    weights, arrived, outs = refs[:3], (refs[3:6], refs[6:9]), refs[9:12]
    buf_gu, buf_d, in_sem, out_sem = refs[12:]
    pieces = [(n, l, s, p) for l in range(2) for s in range(2) for n in range(3) for p in range(2)]
    depth = (buf_gu.shape[0], buf_gu.shape[0], buf_d.shape[0])
    used = [0, 0]
    plan = []
    for n, l, s, p in pieces:
        pool = int(n == 2)
        slot = used[pool] % depth[n]
        prev = used[pool] - depth[n]
        used[pool] += 1
        plan.append((n, l, s, p, pool, slot, prev))
    loads, stores, by_pool = [], [], ([], [])
    for n, l, s, p, pool, slot, prev in plan:
        size = weights[n].shape[2] // 2
        rows = pl.ds(p * size, size)
        buf = (buf_d if pool else buf_gu).at[slot]
        srcs = [weights[n].at[l, s, rows], weights[n].at[l, 1 - s, rows], arrived[l][n].at[rows]]
        loads.append([pltpu.make_async_copy(src, buf, in_sem.at[pool, slot]) for src in srcs])
        stores.append(pltpu.make_async_copy(buf, outs[n].at[l, s, rows], out_sem.at[pool, slot]))
        by_pool[pool].append(stores[-1])
    lag = 6
    for t in range(len(plan) + lag):
        if t < len(plan):
            n, l, s, p, pool, slot, prev = plan[t]
            if prev >= 0:
                by_pool[pool][prev].wait()
            for c, load in enumerate(loads[t]):
                @pl.when(code_ref[l, s] == c)
                def _():
                    load.start()
        if t >= lag:
            loads[t - lag][0].wait()
            stores[t - lag].start()
    for pool in range(2):
        for store in by_pool[pool][-(depth[2 * pool]):]:
            store.wait()


def place_call(code, weights, arrived):
    any_spec = pl.BlockSpec(memory_space=pl.ANY)
    rows_g, cols_g = weights[0].shape[2:]
    rows_d, cols_d = weights[2].shape[2:]
    dt = weights[0].dtype
    return pl.pallas_call(
        place_kernel,
        out_shape=tuple(jax.ShapeDtypeStruct(w.shape, dt) for w in weights),
        in_specs=[pl.BlockSpec(memory_space=pltpu.SMEM)] + [any_spec] * 9,
        out_specs=[any_spec] * 3,
        scratch_shapes=[
            pltpu.VMEM((10, rows_g // 2, cols_g), dt),
            pltpu.VMEM((6, rows_d // 2, cols_d), dt),
            pltpu.SemaphoreType.DMA((2, 10)),
            pltpu.SemaphoreType.DMA((2, 10)),
        ],
        name='place',
    )(code, *weights, *arrived[0], *arrived[1])


def move_weights(weights, old_map, move_slot, move_expert, group, my_dev):
    slots_dev = weights[0].shape[1]
    layers = old_map.shape[0]
    simple, pair, sel, code = move_plan(old_map, move_slot, move_expert, slots_dev, group, my_dev)
    pairs = [None] + [(a, b) for a in range(group) for b in range(a + 1, group)]

    def fast():
        arrived = [lax.switch(pair[l], [functools.partial(swap_call, l, p) for p in pairs], sel[l:l + 1], weights) for l in range(layers)]
        return place_call(code, weights, arrived)

    def slow():
        placed = []
        for l in range(layers):
            layer_w = tuple(w[l] for w in weights)
            outgoing = send_moved(layer_w, old_map[l], move_expert[l], slots_dev, my_dev)
            placed.append(place_moved(layer_w, lax.psum(outgoing, 'ep'), move_slot[l], slots_dev, my_dev))
        return tuple(jnp.stack(parts) for parts in zip(*placed))

    return lax.cond(simple, fast, slow)


def solution(mesh):
    def body(tok_in, routes, gate_vals, w_gate, w_up, w_down, sh_gate, sh_up, sh_down, old_map, move_slot, move_expert):
        my_dev = lax.axis_index('ep')
        slots_dev = w_gate.shape[1]
        hidden = tok_in
        for layer_idx in range(2):
            coefs = slot_coefs(routes[layer_idx], gate_vals[layer_idx], old_map[layer_idx], slots_dev, my_dev)
            hidden = moe_layer(layer_idx, hidden, coefs, (w_gate, w_up, w_down), (sh_gate, sh_up, sh_down))
        new_gate, new_up, new_down = move_weights((w_gate, w_up, w_down), old_map, move_slot, move_expert, mesh.shape['ep'], my_dev)
        return (hidden, new_gate, new_up, new_down)

    weight_spec = P(None, TOKEN_AXES, None, None)
    route_spec = P(None, TOKEN_AXES, None)
    map_spec = P(None, 'replica')
    shared_spec = P(None, None, None)
    tok_spec = P(TOKEN_AXES, None)
    return jax.shard_map(body, mesh=mesh, in_specs=(tok_spec, route_spec, route_spec, weight_spec, weight_spec, weight_spec, shared_spec, shared_spec, shared_spec, map_spec, map_spec, map_spec), out_specs=(tok_spec, weight_spec, weight_spec, weight_spec), check_vma=False)
```
